32 devices in a mesh: dp: 4 (over x, core), ctx: 8 (over z, y).
Axes of the slice: x: 2, y: 2, z: 4, core: 2. Of those that a mesh axis runs over, the one named last changes fastest.
Arguments:
- tokens: bfloat16 [4, 4096, 2048], P('dp', 'ctx'), may hold values from -6 to 6
- in_weight: bfloat16 [2048, 5120], P(None, 'dp'), may hold values from -0.125 to 0.125
- step_weight: bfloat16 [2048, 64], replicated, may hold values from -0.125 to 0.125
- step_bias: float32 [64], replicated, may hold values from -3 to 0
- decay_rate: float32 [64], replicated, may hold values from 0.0001 to 0.5
- skip_gain: float32 [64], replicated, may hold values from 0.5 to 1.5
- filter_taps: float32 [4, 5120], replicated, may hold values from -3 to 3
- filter_bias: float32 [5120], replicated, may hold values from -3 to 3
- norm_gain: float32 [4096], replicated, may hold values from 0.5 to 1.5
Outputs:
- normed: bfloat16 [4, 4096, 4096], P('dp', 'ctx')
The draws below stay inside these ranges and needn't reach their ends.
All inputs are finite; a program needn't handle non-finite values.
Results may differ from the reference program's by a relative error of at most 0.0061.
Values may be sent and summed in bfloat16 or wider, within the bound.
A program may use at most 192 MiB of HBM per device.

```python
import math
import jax
import jax.numpy as jnp
from jax import lax

D = 2048
HEADS = 64
HEAD_DIM = 64
STATE = 128
GROUPS = 4
BLOCK = 256
CONV_K = 4
BATCH = 4
SEQLEN = 4096
XBC = 5120


def steps_of(rng, dims, shards, low, largest):
    level, own = 1.0, jax.random.fold_in(rng, 6)
    for axis_at, shards_of in shards:
        steps = jnp.exp(jax.random.uniform(jax.random.fold_in(own, axis_at), (shards_of,), jnp.float32, low / len(shards), largest / len(shards)))
        level = level * jnp.repeat(steps, dims[axis_at] // shards_of).reshape([-1 if axis == axis_at else 1 for axis in range(len(dims))])
    return level


def bell_draw(key, extent, scale, bound, shards=(), held_as=jnp.bfloat16):
    values = scale * jax.random.normal(key, extent, jnp.float32)
    if shards:
        values = values * steps_of(key, extent, shards, -0.22, 0.18)
    return jnp.clip(values, -bound, bound).astype(held_as)


def setup_inputs(seed: int = 0) -> dict:
    streams_of = jax.random.split(jax.random.key(seed), 10)
    return {
        "tokens": bell_draw(streams_of[0], (BATCH, SEQLEN, D), 1.0, 6.0, ((0, 4), (1, 8))),
        "in_weight": bell_draw(streams_of[1], (D, XBC), D ** -0.5, 0.125, ((1, 4),)),
        "step_weight": bell_draw(streams_of[2], (D, HEADS), D ** -0.5, 0.125),
        "step_bias": jnp.clip(jax.random.uniform(streams_of[3], (HEADS,), jnp.float32, -3.0, 0.0), -3.0, 0.0),
        "decay_rate": jnp.clip(jnp.exp(jax.random.uniform(streams_of[4], (HEADS,), jnp.float32, math.log(0.0001), math.log(0.5))), 0.0001, 0.5),
        "skip_gain": jnp.clip(jax.random.uniform(streams_of[5], (HEADS,), jnp.float32, 0.5, 1.5), 0.5, 1.5),
        "filter_taps": bell_draw(streams_of[6], (CONV_K, XBC), CONV_K ** -0.5, 3.0, (), jnp.float32),
        "filter_bias": bell_draw(streams_of[7], (XBC,), 0.5, 3.0, (), jnp.float32),
        "norm_gain": jnp.clip(jax.random.uniform(streams_of[8], (HEADS * HEAD_DIM,), jnp.float32, 0.5, 1.5), 0.5, 1.5),
    }


def filter_rows(prefix, current, filter_taps, filter_bias):
    padded = jnp.concatenate([prefix, current], axis=0).astype(jnp.float32)
    length = current.shape[0]
    summed = filter_bias + filter_taps[0] * padded[0:length]
    for offset in range(1, filter_taps.shape[0]):
        summed = summed + filter_taps[offset] * padded[offset:offset + length]
    return summed

def ssd_group(values, input_map, output_map, step_size, decay_rate, skip_gain, block_len):
    length, head_count, head_width = values.shape
    block_count = length // block_len
    bundle = math.gcd(block_count, 8)
    bundle_count = block_count // bundle
    highest = lax.Precision.HIGHEST
    value_rows = values.reshape(block_count, block_len, head_count, head_width)
    input_rows = input_map.reshape(block_count, block_len, -1)
    output_rows = output_map.reshape(block_count, block_len, -1)
    step_rows = step_size.reshape(block_count, block_len, head_count)
    decay_sum = jnp.cumsum(-step_rows * decay_rate, axis=1)
    causal = (jnp.arange(block_len)[:, None] >= jnp.arange(block_len)[None, :])[None, :, :, None]

    def local_block(pieces):
        value_block, input_block, output_block, step_block, decay_block = pieces
        value_wide = value_block.astype(jnp.float32)
        input_wide = input_block.astype(jnp.float32)
        scores = jnp.einsum('ktn,kun->ktu', output_block.astype(jnp.float32), input_wide, precision=highest)
        decay_gap = jnp.where(causal, decay_block[:, :, None, :] - decay_block[:, None, :, :], 0.0)
        weights = jnp.where(causal, jnp.exp(decay_gap), 0.0) * scores[..., None] * step_block[:, None, :, :]
        weights = weights.astype(jnp.bfloat16).astype(jnp.float32)
        within = jnp.einsum('ktuh,kuhp->kthp', weights, value_wide, precision=highest)
        to_end = jnp.exp(decay_block[:, -1:, :] - decay_block) * step_block
        scaled = (to_end[..., None] * value_wide).astype(jnp.bfloat16).astype(jnp.float32)
        states = jnp.einsum('kuhp,kun->khpn', scaled, input_wide, precision=highest)
        return (within, states)

    def blocked(array):
        return array.reshape((bundle_count, bundle) + array.shape[1:])
    within, states = lax.map(local_block, (blocked(value_rows), blocked(input_rows), blocked(output_rows), blocked(step_rows), blocked(decay_sum)))
    within = within.reshape(block_count, block_len, head_count, head_width)
    states = states.reshape((block_count,) + states.shape[2:])
    totals = decay_sum[:, -1, :]
    running = jnp.cumsum(totals, axis=0)
    starts = running - totals
    before = (jnp.arange(block_count)[:, None] > jnp.arange(block_count)[None, :])[:, :, None]
    mixing = jnp.where(before, jnp.exp(jnp.where(before, starts[:, None, :] - running[None, :, :], 0.0)), 0.0)
    entering = jnp.einsum('kjh,jhpn->khpn', mixing, states, precision=highest)
    carried = jnp.einsum('khpn,ktn->kthp', entering, output_rows.astype(jnp.float32), precision=highest) * jnp.exp(decay_sum)[..., None]
    output = within + carried + skip_gain[:, None] * value_rows.astype(jnp.float32)
    return output.reshape(length, head_count, head_width)

def group_norm(values, norm_gain):
    length = values.shape[0]
    grouped = values.astype(jnp.float32).reshape(length, GROUPS, -1)
    mean_square = lax.optimization_barrier(jnp.mean(jnp.square(grouped), axis=-1, keepdims=True))
    return (grouped * lax.rsqrt(mean_square + 1e-05)).reshape(length, -1) * norm_gain

def reference(tokens, in_weight, step_weight, step_bias, decay_rate, skip_gain, filter_taps, filter_bias, norm_gain):
    inner_width = HEADS * HEAD_DIM
    map_width = GROUPS * STATE
    group_heads = HEADS // GROUPS
    results = []
    for member in range(BATCH):
        token_rows = tokens[member]
        projected = jnp.dot(token_rows, in_weight, preferred_element_type=jnp.float32).astype(jnp.bfloat16)
        step_raw = jnp.dot(token_rows, step_weight, preferred_element_type=jnp.float32).astype(jnp.bfloat16)
        prefix = jnp.zeros((CONV_K - 1, projected.shape[1]), jnp.bfloat16)
        active = jax.nn.silu(filter_rows(prefix, projected, filter_taps, filter_bias)).astype(jnp.bfloat16)
        step_size = jax.nn.softplus(step_raw.astype(jnp.float32) + step_bias)
        inputs = active[:, :inner_width].reshape(SEQLEN, HEADS, HEAD_DIM)
        outputs = []
        for group_index in range(GROUPS):
            heads_here = slice(group_index * group_heads, (group_index + 1) * group_heads)
            first_in = inner_width + group_index * STATE
            first_out = inner_width + map_width + group_index * STATE
            outputs.append(ssd_group(inputs[:, heads_here], active[:, first_in:first_in + STATE], active[:, first_out:first_out + STATE], step_size[:, heads_here], decay_rate[heads_here], skip_gain[heads_here], BLOCK))
        mixed_rows = jnp.concatenate(outputs, axis=1).reshape(SEQLEN, inner_width).astype(jnp.bfloat16)
        results.append(group_norm(mixed_rows, norm_gain).astype(jnp.bfloat16))
    return jnp.stack(results)
```

```python
import functools
import math

import jax
import jax.numpy as jnp
from jax import lax
from jax.experimental import pallas as pl
from jax.experimental.pallas import tpu as pltpu
from jax.sharding import PartitionSpec as P

HEADS = 64
HEAD_DIM = 64
STATE = 128
GROUPS = 4
BLOCK = 256
GROUP_HEADS = HEADS // GROUPS
GROUP_WIDTH = GROUP_HEADS * HEAD_DIM
INNER = HEADS * HEAD_DIM
RIM = 16
LOG2E = math.log2(math.e)
VMEM_LIMIT = 60 * 2**20


def project_kernel(rows_ref, weight_ref, taps_ref, bias_ref, active_ref):
    length = active_ref.shape[0]
    projected = jnp.dot(rows_ref[...], weight_ref[0], preferred_element_type=jnp.float32)
    projected = projected.astype(jnp.bfloat16).astype(jnp.float32)
    taps = taps_ref[...]
    count = taps.shape[0]
    summed = bias_ref[...] + taps[count - 1 : count] * projected[RIM:]
    for k in range(count - 1):
        first = RIM - (count - 1) + k
        summed = summed + taps[k : k + 1] * projected[first : first + length]
    active_ref[...] = (summed / (1.0 + jnp.exp(-summed))).astype(jnp.bfloat16)


def project(rows, weight, taps, bias, tile):
    length = rows.shape[0] - RIM
    shards, depth, width = weight.shape
    tiles = width // tile
    column = lambda s, j: (0, s * tiles + j)
    return pl.pallas_call(
        project_kernel,
        grid=(shards, tiles),
        in_specs=[
            pl.BlockSpec(rows.shape, lambda s, j: (0, 0)),
            pl.BlockSpec((1, depth, tile), lambda s, j: (s, 0, j)),
            pl.BlockSpec((taps.shape[0], tile), column),
            pl.BlockSpec((1, tile), column),
        ],
        out_specs=pl.BlockSpec((length, tile), column),
        out_shape=jax.ShapeDtypeStruct((length, shards * width), jnp.bfloat16),
        compiler_params=pltpu.CompilerParams(vmem_limit_bytes=VMEM_LIMIT),
        name="project",
    )(rows, weight, taps, bias)


def pair_columns(columns, pair, low_half):
    first = 2 * pair
    return jnp.where(low_half, columns[:, first : first + 1], columns[:, first + 1 : first + 2])


def block_state(values, input_map, ending, gap_columns, low_half):
    pieces = []
    for pair in range(GROUP_HEADS // 2):
        lanes = slice(pair * 128, (pair + 1) * 128)
        weight = jnp.exp2(ending[:, lanes] - pair_columns(gap_columns, pair, low_half))
        pieces.append((weight * values[:, lanes].astype(jnp.float32)).astype(jnp.bfloat16))
    scaled = jnp.concatenate(pieces, axis=1)
    return lax.dot_general(
        input_map, scaled, (((0,), (0,)), ((), ())), preferred_element_type=jnp.float32
    )


def low_mask(rows):
    return lax.broadcasted_iota(jnp.int32, (rows, 128), 1) < HEAD_DIM


def states_kernel(values_ref, input_ref, gap_ref, ending_ref, state_ref):
    blocks = values_ref.shape[0] // BLOCK
    low_half = low_mask(BLOCK)
    total = None
    for k in range(blocks):
        rows = pl.ds(k * BLOCK, BLOCK)
        ending = ending_ref[k]
        state = block_state(values_ref[rows, :], input_ref[rows, :], ending, gap_ref[0, rows, :], low_half)
        total = state if total is None else total * jnp.exp2(ending) + state
    chunks, _, width = state_ref.shape
    for chunk in range(chunks):
        state_ref[chunk] = total[:, chunk * width : (chunk + 1) * width].astype(jnp.bfloat16)


def device_states(active, gap, ending, parts):
    length = active.shape[0]
    chunks = parts // GROUPS
    blocks = length // BLOCK
    width = INNER // parts
    return pl.pallas_call(
        states_kernel,
        grid=(GROUPS,),
        in_specs=[
            pl.BlockSpec((length, GROUP_WIDTH), lambda g: (0, g)),
            pl.BlockSpec((length, STATE), lambda g: (0, INNER // STATE + g)),
            pl.BlockSpec((1, length, GROUP_HEADS), lambda g: (g, 0, 0)),
            pl.BlockSpec((blocks, 1, GROUP_WIDTH), lambda g: (0, 0, g)),
        ],
        out_specs=pl.BlockSpec((chunks, STATE, width), lambda g: (g, 0, 0)),
        out_shape=jax.ShapeDtypeStruct((parts, STATE, width), jnp.bfloat16),
        compiler_params=pltpu.CompilerParams(vmem_limit_bytes=VMEM_LIMIT),
        name="states",
    )(active, active, gap, ending)


def mix_kernel(
    values_ref,
    input_ref,
    output_ref,
    decay_ref,
    gap_ref,
    gap_row_ref,
    ending_ref,
    entering_ref,
    skip_ref,
    gain_ref,
    normed_ref,
    entering_scratch,
    mixed_scratch,
):
    blocks = values_ref.shape[0] // BLOCK
    half = BLOCK // 2
    low_half = low_mask(BLOCK)
    causal = lax.broadcasted_iota(jnp.int32, (half, half), 0) >= lax.broadcasted_iota(
        jnp.int32, (half, half), 1
    )
    chunks, _, width = entering_ref.shape
    for chunk in range(chunks):
        entering_scratch[:, chunk * width : (chunk + 1) * width] = entering_ref[chunk].astype(jnp.float32)
    for k in range(blocks):
        rows = pl.ds(k * BLOCK, BLOCK)
        input_map = input_ref[rows, :]
        output_map = output_ref[rows, :]
        scores = lax.dot_general(
            output_map, input_map, (((1,), (1,)), ((), ())), preferred_element_type=jnp.float32
        )
        decay = decay_ref[0, rows, :]
        gap_rows = gap_row_ref[0, :, rows]
        carried = jnp.dot(
            output_map, entering_scratch[...].astype(jnp.bfloat16), preferred_element_type=jnp.float32
        )
        squares = jnp.zeros((BLOCK, 128), jnp.float32)
        for pair in range(GROUP_HEADS // 2):
            lanes = slice(pair * 128, (pair + 1) * 128)
            values = values_ref[rows, lanes]
            within = []
            for head in (2 * pair, 2 * pair + 1):
                column = decay[:, head : head + 1]
                row = gap_rows[head : head + 1, :]
                top = jnp.where(causal, column[:half] - row[:, :half], -jnp.inf)
                top = (jnp.exp2(top) * scores[:half, :half]).astype(jnp.bfloat16)
                left = jnp.exp2(column[half:] - row[:, :half]) * scores[half:, :half]
                right = jnp.where(causal, column[half:] - row[:, half:], -jnp.inf)
                right = jnp.exp2(right) * scores[half:, half:]
                bottom = jnp.concatenate([left, right], axis=1).astype(jnp.bfloat16)
                within.append(
                    jnp.concatenate(
                        [
                            jnp.dot(top, values[:half], preferred_element_type=jnp.float32),
                            jnp.dot(bottom, values, preferred_element_type=jnp.float32),
                        ],
                        axis=0,
                    )
                )
            inside = jnp.where(low_half, within[0], within[1])
            growth = jnp.exp2(pair_columns(decay, pair, low_half))
            mixed = (
                inside
                + growth * carried[:, lanes]
                + skip_ref[:, lanes] * values.astype(jnp.float32)
            ).astype(jnp.bfloat16)
            mixed_scratch[:, lanes] = mixed
            wide = mixed.astype(jnp.float32)
            squares = squares + wide * wide
        mean = jnp.sum(squares, axis=1, keepdims=True) * (1.0 / GROUP_WIDTH)
        scale = lax.rsqrt(mean + 1e-05)
        normed_ref[rows, :] = (
            mixed_scratch[...].astype(jnp.float32) * scale * gain_ref[...]
        ).astype(jnp.bfloat16)
        if k < blocks - 1:
            ending = ending_ref[k]
            state = block_state(values_ref[rows, :], input_map, ending, gap_ref[0, rows, :], low_half)
            entering_scratch[...] = entering_scratch[...] * jnp.exp2(ending) + state


def mix(active, decay, gap, gap_rows, ending, entering, skip, gain):
    length = active.shape[0]
    blocks = length // BLOCK
    parts, _, width = entering.shape
    chunks = parts // GROUPS
    group_column = lambda g: (0, g)
    return pl.pallas_call(
        mix_kernel,
        grid=(GROUPS,),
        in_specs=[
            pl.BlockSpec((length, GROUP_WIDTH), group_column),
            pl.BlockSpec((length, STATE), lambda g: (0, INNER // STATE + g)),
            pl.BlockSpec((length, STATE), lambda g: (0, INNER // STATE + GROUPS + g)),
            pl.BlockSpec((1, length, GROUP_HEADS), lambda g: (g, 0, 0)),
            pl.BlockSpec((1, length, GROUP_HEADS), lambda g: (g, 0, 0)),
            pl.BlockSpec((1, GROUP_HEADS, length), lambda g: (g, 0, 0)),
            pl.BlockSpec((blocks, 1, GROUP_WIDTH), lambda g: (0, 0, g)),
            pl.BlockSpec((chunks, STATE, width), lambda g: (g, 0, 0)),
            pl.BlockSpec((1, GROUP_WIDTH), group_column),
            pl.BlockSpec((1, GROUP_WIDTH), group_column),
        ],
        out_specs=pl.BlockSpec((length, GROUP_WIDTH), group_column),
        out_shape=jax.ShapeDtypeStruct((length, INNER), jnp.bfloat16),
        scratch_shapes=[
            pltpu.VMEM((STATE, GROUP_WIDTH), jnp.float32),
            pltpu.VMEM((BLOCK, GROUP_WIDTH), jnp.bfloat16),
        ],
        compiler_params=pltpu.CompilerParams(vmem_limit_bytes=VMEM_LIMIT),
        name="mix",
    )(active, active, active, decay, gap, gap_rows, ending, entering, skip, gain)


def per_device(
    tokens,
    in_weight,
    step_weight,
    step_bias,
    decay_rate,
    skip_gain,
    filter_taps,
    filter_bias,
    norm_gain,
):
    token_rows = tokens[0]
    length = token_rows.shape[0]
    blocks = length // BLOCK
    parts = lax.axis_size("ctx")
    weight = lax.all_gather(in_weight, "dp")
    rim = lax.ppermute(token_rows[length - RIM :], "ctx", [(s, s + 1) for s in range(parts - 1)])
    rows = jnp.concatenate([rim, token_rows], axis=0)

    step_raw = jnp.dot(token_rows, step_weight, preferred_element_type=jnp.float32).astype(
        jnp.bfloat16
    )
    step_size = jax.nn.softplus(step_raw.astype(jnp.float32) + step_bias)
    decay = jnp.cumsum((-step_size * decay_rate).reshape(blocks, BLOCK, HEADS), axis=1) * LOG2E
    ending = decay[:, -1, :]
    decay = decay.reshape(length, HEADS)
    gap = decay - jnp.log2(step_size)
    grouped = lambda array: array.reshape(length, GROUPS, GROUP_HEADS).transpose(1, 0, 2)
    decay_columns, gap_columns = grouped(decay), grouped(gap)
    gap_rows = gap.T.reshape(GROUPS, GROUP_HEADS, length)
    ending_lanes = jnp.repeat(ending, HEAD_DIM, axis=1)[:, None, :]
    totals = lax.all_gather(jnp.sum(ending, axis=0), "ctx")
    mine = lax.axis_index("ctx")
    heads_each = HEADS // parts
    totals = lax.dynamic_slice_in_dim(totals, mine * heads_each, heads_each, 1)
    factors = jnp.repeat(jnp.exp2(totals), HEAD_DIM, axis=1)[:, None, :]

    active = project(rows, weight, filter_taps, filter_bias[None], 256)
    states = device_states(active, gap_columns, ending_lanes, parts)
    owned = lax.all_to_all(states, "ctx", split_axis=0, concat_axis=0, tiled=True)
    running = jnp.zeros(owned.shape[1:], jnp.float32)
    entering = []
    for source in range(parts):
        entering.append(running.astype(jnp.bfloat16))
        running = running * factors[source] + owned[source].astype(jnp.float32)
    entering = lax.all_to_all(jnp.stack(entering), "ctx", split_axis=0, concat_axis=0, tiled=True)
    skip = jnp.repeat(skip_gain, HEAD_DIM)[None]
    return mix(
        active, decay_columns, gap_columns, gap_rows, ending_lanes, entering, skip, norm_gain[None]
    )[None]


def solution(mesh):
    in_specs = (P("dp", "ctx", None), P(None, "dp"), P(), P(), P(), P(), P(), P(), P())
    out_specs = P("dp", "ctx", None)
    return jax.shard_map(
        per_device, mesh=mesh, in_specs=in_specs, out_specs=out_specs, check_vma=False
    )
```

```python
import functools
import math

import jax
import jax.numpy as jnp
from jax import lax
from jax.experimental import pallas as pl
from jax.experimental.pallas import tpu as pltpu
from jax.sharding import PartitionSpec as P

HEADS = 64
HEAD_DIM = 64
STATE = 128
GROUPS = 4
BLOCK = 256
GROUP_HEADS = HEADS // GROUPS
GROUP_WIDTH = GROUP_HEADS * HEAD_DIM
INNER = HEADS * HEAD_DIM
RIM = 16
LOG2E = math.log2(math.e)
VMEM_LIMIT = 60 * 2**20


CHUNKS = 4
SENT_ORDER = (2, 3, 0, 1)
TILE = 256


def flipped(index, bit):
    return index + bit - 2 * bit * ((index // bit) % 2)


def gather_project_kernel(
    rows_ref,
    weight_ref,
    taps_ref,
    bias_ref,
    active_ref,
    held,
    sums,
    local_sem,
    own_send,
    own_recv,
    x_send,
    x_recv,
    y_send,
    y_recv,
    z_send,
    z_recv,
    core_send,
    core_recv,
):
    me_dp, me_ctx = lax.axis_index("dp"), lax.axis_index("ctx")
    depth, width = weight_ref.shape
    length = active_ref.shape[0]
    quarter = depth // 4
    piece = quarter // CHUNKS
    partner, across, beyond = flipped(me_dp, 1), flipped(me_dp, 2), flipped(flipped(me_dp, 1), 2)
    core_peer, x_peer = (partner, me_ctx), (across, me_ctx)
    y_peer, z_peer = (me_dp, flipped(me_ctx, 1)), (me_dp, flipped(me_ctx, 2))
    mine = me_ctx % 4
    quarters = (mine, flipped(mine, 1), flipped(mine, 2), 3 - mine)

    barrier = pltpu.get_barrier_semaphore()
    for peer in (core_peer, x_peer, y_peer, z_peer):
        pl.semaphore_signal(
            barrier, inc=1, device_id=peer, device_id_type=pl.DeviceIdType.MESH
        )
    pl.semaphore_wait(barrier, 4)

    def span(kind, chunk):
        start = quarters[kind] * quarter + chunk * piece
        return pl.ds(pl.multiple_of(start, piece), piece)

    def remote(source, target, send, recv, peer):
        return pltpu.make_async_remote_copy(
            src_ref=source,
            dst_ref=target,
            send_sem=send,
            recv_sem=recv,
            device_id=peer,
            device_id_type=pl.DeviceIdType.MESH,
        )

    started = []

    def start(copy):
        copy.start()
        started.append(copy)

    local = pltpu.make_async_copy(weight_ref, held.at[me_dp], local_sem)
    local.start()
    start(remote(weight_ref, held.at[me_dp], own_send, own_recv, core_peer))
    x_slots = [(0, chunk) for chunk in SENT_ORDER] + [(3, 0), (3, 1)]
    for slot, (kind, chunk) in enumerate(x_slots):
        rows = span(kind, chunk)
        start(
            remote(
                weight_ref.at[rows, :],
                held.at[me_dp, rows, :],
                x_send.at[slot],
                x_recv.at[slot],
                x_peer,
            )
        )

    def landed(kind, chunk, recv, send, peer):
        part = held.at[across, span(kind, chunk), :]
        remote(part, part, send, recv, peer).wait_recv()

    def forward(kind, chunk, send, recv, peer):
        part = held.at[across, span(kind, chunk), :]
        start(remote(part, part, send, recv, peer))

    def to_core(kind, chunk):
        slot = kind * CHUNKS + chunk
        forward(kind, chunk, core_send.at[slot], core_recv.at[slot], core_peer)

    def from_x(slot):
        kind, chunk = x_slots[slot]
        landed(kind, chunk, x_recv.at[slot], x_send.at[slot], x_peer)
        if slot < CHUNKS:
            forward(kind, chunk, y_send.at[slot], y_recv.at[slot], y_peer)
            forward(kind, chunk, z_send.at[slot], z_recv.at[slot], z_peer)
        to_core(kind, chunk)

    def from_y(slot):
        kind, chunk = (1, SENT_ORDER[slot]) if slot < CHUNKS else (3, 3)
        landed(kind, chunk, y_recv.at[slot], y_send.at[slot], y_peer)
        if (kind, chunk) == (1, 2):
            forward(kind, chunk, z_send.at[CHUNKS], z_recv.at[CHUNKS], z_peer)
        to_core(kind, chunk)

    def from_z(slot):
        kind, chunk = (2, SENT_ORDER[slot]) if slot < CHUNKS else (3, 2)
        landed(kind, chunk, z_recv.at[slot], z_send.at[slot], z_peer)
        if (kind, chunk) == (2, 3):
            forward(kind, chunk, y_send.at[CHUNKS], y_recv.at[CHUNKS], y_peer)
        to_core(kind, chunk)

    def from_core(kind):
        for chunk in range(CHUNKS):
            part = held.at[beyond, span(kind, chunk), :]
            slot = kind * CHUNKS + chunk
            remote(part, part, core_send.at[slot], core_recv.at[slot], core_peer).wait_recv()

    def finish(total, shard, tile):
        lanes = pl.ds(pl.multiple_of(shard * width + tile * TILE, 128), TILE)
        projected = total.astype(jnp.bfloat16).astype(jnp.float32)
        taps = taps_ref[:, lanes]
        count = taps.shape[0]
        summed = bias_ref[:, lanes] + taps[count - 1 : count] * projected[RIM:]
        for k in range(count - 1):
            first = RIM - (count - 1) + k
            summed = summed + taps[k : k + 1] * projected[first : first + length]
        active_ref[:, lanes] = (summed / (1.0 + jnp.exp(-summed))).astype(jnp.bfloat16)

    def whole_shard(shard):
        @pl.loop(0, width // TILE)
        def _(tile):
            lanes = pl.ds(pl.multiple_of(tile * TILE, TILE), TILE)
            finish(
                jnp.dot(
                    rows_ref[...], held[shard, :, lanes], preferred_element_type=jnp.float32
                ),
                shard,
                tile,
            )

    def part_shard(shard, at, kinds, first, last):
        @pl.loop(0, width // TILE)
        def _(tile):
            lanes = pl.ds(pl.multiple_of(tile * TILE, TILE), TILE)
            total = None if first else sums[at, :, lanes]
            for kind in kinds:
                deep = pl.ds(pl.multiple_of(quarters[kind] * quarter, quarter), quarter)
                product = jnp.dot(
                    rows_ref[:, deep],
                    held[shard, deep, lanes],
                    preferred_element_type=jnp.float32,
                )
                total = product if total is None else total + product
            if last:
                finish(total, shard, tile)
            else:
                sums[at, :, lanes] = total

    local.wait()
    whole_shard(me_dp)
    from_x(0)
    remote(weight_ref, held.at[partner], own_send, own_recv, core_peer).wait_recv()
    whole_shard(partner)
    from_x(1)
    from_y(0)
    from_z(0)
    from_x(2)
    from_z(1)
    from_y(1)
    from_x(3)
    part_shard(across, 0, (0,), True, False)
    from_core(0)
    part_shard(beyond, 1, (0,), True, False)
    from_y(2)
    from_z(2)
    from_y(3)
    from_z(3)
    part_shard(across, 0, (1, 2), False, False)
    from_core(1)
    from_core(2)
    part_shard(beyond, 1, (1, 2), False, False)
    from_x(4)
    from_x(5)
    from_y(4)
    from_z(4)
    part_shard(across, 0, (3,), False, True)
    from_core(3)
    part_shard(beyond, 1, (3,), False, True)
    for copy in started:
        copy.wait_send()


def gather_project(rows, weight, taps, bias):
    length = rows.shape[0] - RIM
    depth, width = weight.shape
    shards = lax.axis_size("dp")
    dma = pltpu.SemaphoreType.DMA
    vmem = pl.BlockSpec(memory_space=pltpu.VMEM)
    return pl.pallas_call(
        gather_project_kernel,
        in_specs=[vmem, pl.BlockSpec(memory_space=pl.ANY), vmem, vmem],
        out_specs=vmem,
        out_shape=jax.ShapeDtypeStruct((length, shards * width), jnp.bfloat16),
        scratch_shapes=[
            pltpu.VMEM((shards, depth, width), jnp.bfloat16),
            pltpu.VMEM((2, length + RIM, width), jnp.float32),
            dma,
            dma,
            dma,
            dma((CHUNKS + 2,)),
            dma((CHUNKS + 2,)),
            dma((CHUNKS + 1,)),
            dma((CHUNKS + 1,)),
            dma((CHUNKS + 1,)),
            dma((CHUNKS + 1,)),
            dma((4 * CHUNKS,)),
            dma((4 * CHUNKS,)),
        ],
        compiler_params=pltpu.CompilerParams(
            vmem_limit_bytes=VMEM_LIMIT, collective_id=0, has_side_effects=True
        ),
        name="gather_project",
    )(rows, weight, taps, bias)


def pair_columns(columns, pair, low_half):
    first = 2 * pair
    return jnp.where(low_half, columns[:, first : first + 1], columns[:, first + 1 : first + 2])


def block_state(values, input_map, ending, gap_columns, low_half):
    pieces = []
    for pair in range(GROUP_HEADS // 2):
        lanes = slice(pair * 128, (pair + 1) * 128)
        weight = jnp.exp2(ending[:, lanes] - pair_columns(gap_columns, pair, low_half))
        pieces.append((weight * values[:, lanes].astype(jnp.float32)).astype(jnp.bfloat16))
    scaled = jnp.concatenate(pieces, axis=1)
    return lax.dot_general(
        input_map, scaled, (((0,), (0,)), ((), ())), preferred_element_type=jnp.float32
    )


def low_mask(rows):
    return lax.broadcasted_iota(jnp.int32, (rows, 128), 1) < HEAD_DIM


def states_kernel(values_ref, input_ref, gap_ref, ending_ref, state_ref):
    blocks = values_ref.shape[0] // BLOCK
    low_half = low_mask(BLOCK)
    total = None
    for k in range(blocks):
        rows = pl.ds(k * BLOCK, BLOCK)
        ending = ending_ref[k]
        state = block_state(values_ref[rows, :], input_ref[rows, :], ending, gap_ref[0, rows, :], low_half)
        total = state if total is None else total * jnp.exp2(ending) + state
    chunks, _, width = state_ref.shape
    for chunk in range(chunks):
        state_ref[chunk] = total[:, chunk * width : (chunk + 1) * width].astype(jnp.bfloat16)


def device_states(active, gap, ending, parts):
    length = active.shape[0]
    chunks = parts // GROUPS
    blocks = length // BLOCK
    width = INNER // parts
    return pl.pallas_call(
        states_kernel,
        grid=(GROUPS,),
        in_specs=[
            pl.BlockSpec((length, GROUP_WIDTH), lambda g: (0, g)),
            pl.BlockSpec((length, STATE), lambda g: (0, INNER // STATE + g)),
            pl.BlockSpec((1, length, GROUP_HEADS), lambda g: (g, 0, 0)),
            pl.BlockSpec((blocks, 1, GROUP_WIDTH), lambda g: (0, 0, g)),
        ],
        out_specs=pl.BlockSpec((chunks, STATE, width), lambda g: (g, 0, 0)),
        out_shape=jax.ShapeDtypeStruct((parts, STATE, width), jnp.bfloat16),
        compiler_params=pltpu.CompilerParams(vmem_limit_bytes=VMEM_LIMIT),
        name="states",
    )(active, active, gap, ending)


def mix_kernel(
    values_ref,
    input_ref,
    output_ref,
    decay_ref,
    gap_ref,
    gap_row_ref,
    ending_ref,
    entering_ref,
    skip_ref,
    gain_ref,
    normed_ref,
    entering_scratch,
    mixed_scratch,
):
    blocks = values_ref.shape[0] // BLOCK
    half = BLOCK // 2
    low_half = low_mask(BLOCK)
    causal = lax.broadcasted_iota(jnp.int32, (half, half), 0) >= lax.broadcasted_iota(
        jnp.int32, (half, half), 1
    )
    chunks, _, width = entering_ref.shape
    for chunk in range(chunks):
        entering_scratch[:, chunk * width : (chunk + 1) * width] = entering_ref[chunk].astype(jnp.float32)
    for k in range(blocks):
        rows = pl.ds(k * BLOCK, BLOCK)
        input_map = input_ref[rows, :]
        output_map = output_ref[rows, :]
        scores = lax.dot_general(
            output_map, input_map, (((1,), (1,)), ((), ())), preferred_element_type=jnp.float32
        )
        decay = decay_ref[0, rows, :]
        gap_rows = gap_row_ref[0, :, rows]
        carried = jnp.dot(
            output_map, entering_scratch[...].astype(jnp.bfloat16), preferred_element_type=jnp.float32
        )
        squares = jnp.zeros((BLOCK, 128), jnp.float32)
        for pair in range(GROUP_HEADS // 2):
            lanes = slice(pair * 128, (pair + 1) * 128)
            values = values_ref[rows, lanes]
            within = []
            for head in (2 * pair, 2 * pair + 1):
                column = decay[:, head : head + 1]
                row = gap_rows[head : head + 1, :]
                top = jnp.where(causal, column[:half] - row[:, :half], -jnp.inf)
                top = (jnp.exp2(top) * scores[:half, :half]).astype(jnp.bfloat16)
                left = jnp.exp2(column[half:] - row[:, :half]) * scores[half:, :half]
                right = jnp.where(causal, column[half:] - row[:, half:], -jnp.inf)
                right = jnp.exp2(right) * scores[half:, half:]
                bottom = jnp.concatenate([left, right], axis=1).astype(jnp.bfloat16)
                within.append(
                    jnp.concatenate(
                        [
                            jnp.dot(top, values[:half], preferred_element_type=jnp.float32),
                            jnp.dot(bottom, values, preferred_element_type=jnp.float32),
                        ],
                        axis=0,
                    )
                )
            inside = jnp.where(low_half, within[0], within[1])
            growth = jnp.exp2(pair_columns(decay, pair, low_half))
            mixed = (
                inside
                + growth * carried[:, lanes]
                + skip_ref[:, lanes] * values.astype(jnp.float32)
            ).astype(jnp.bfloat16)
            mixed_scratch[:, lanes] = mixed
            wide = mixed.astype(jnp.float32)
            squares = squares + wide * wide
        mean = jnp.sum(squares, axis=1, keepdims=True) * (1.0 / GROUP_WIDTH)
        scale = lax.rsqrt(mean + 1e-05)
        normed_ref[rows, :] = (
            mixed_scratch[...].astype(jnp.float32) * scale * gain_ref[...]
        ).astype(jnp.bfloat16)
        if k < blocks - 1:
            ending = ending_ref[k]
            state = block_state(values_ref[rows, :], input_map, ending, gap_ref[0, rows, :], low_half)
            entering_scratch[...] = entering_scratch[...] * jnp.exp2(ending) + state


def mix(active, decay, gap, gap_rows, ending, entering, skip, gain):
    length = active.shape[0]
    blocks = length // BLOCK
    parts, _, width = entering.shape
    chunks = parts // GROUPS
    group_column = lambda g: (0, g)
    return pl.pallas_call(
        mix_kernel,
        grid=(GROUPS,),
        in_specs=[
            pl.BlockSpec((length, GROUP_WIDTH), group_column),
            pl.BlockSpec((length, STATE), lambda g: (0, INNER // STATE + g)),
            pl.BlockSpec((length, STATE), lambda g: (0, INNER // STATE + GROUPS + g)),
            pl.BlockSpec((1, length, GROUP_HEADS), lambda g: (g, 0, 0)),
            pl.BlockSpec((1, length, GROUP_HEADS), lambda g: (g, 0, 0)),
            pl.BlockSpec((1, GROUP_HEADS, length), lambda g: (g, 0, 0)),
            pl.BlockSpec((blocks, 1, GROUP_WIDTH), lambda g: (0, 0, g)),
            pl.BlockSpec((chunks, STATE, width), lambda g: (g, 0, 0)),
            pl.BlockSpec((1, GROUP_WIDTH), group_column),
            pl.BlockSpec((1, GROUP_WIDTH), group_column),
        ],
        out_specs=pl.BlockSpec((length, GROUP_WIDTH), group_column),
        out_shape=jax.ShapeDtypeStruct((length, INNER), jnp.bfloat16),
        scratch_shapes=[
            pltpu.VMEM((STATE, GROUP_WIDTH), jnp.float32),
            pltpu.VMEM((BLOCK, GROUP_WIDTH), jnp.bfloat16),
        ],
        compiler_params=pltpu.CompilerParams(vmem_limit_bytes=VMEM_LIMIT),
        name="mix",
    )(active, active, active, decay, gap, gap_rows, ending, entering, skip, gain)


def per_device(
    tokens,
    in_weight,
    step_weight,
    step_bias,
    decay_rate,
    skip_gain,
    filter_taps,
    filter_bias,
    norm_gain,
):
    token_rows = tokens[0]
    length = token_rows.shape[0]
    blocks = length // BLOCK
    parts = lax.axis_size("ctx")
    rim = lax.ppermute(token_rows[length - RIM :], "ctx", [(s, s + 1) for s in range(parts - 1)])
    rows = jnp.concatenate([rim, token_rows], axis=0)

    step_raw = jnp.dot(token_rows, step_weight, preferred_element_type=jnp.float32).astype(
        jnp.bfloat16
    )
    step_size = jax.nn.softplus(step_raw.astype(jnp.float32) + step_bias)
    decay = jnp.cumsum((-step_size * decay_rate).reshape(blocks, BLOCK, HEADS), axis=1) * LOG2E
    ending = decay[:, -1, :]
    decay = decay.reshape(length, HEADS)
    gap = decay - jnp.log2(step_size)
    grouped = lambda array: array.reshape(length, GROUPS, GROUP_HEADS).transpose(1, 0, 2)
    decay_columns, gap_columns = grouped(decay), grouped(gap)
    gap_rows = gap.T.reshape(GROUPS, GROUP_HEADS, length)
    ending_lanes = jnp.repeat(ending, HEAD_DIM, axis=1)[:, None, :]
    totals = lax.all_gather(jnp.sum(ending, axis=0), "ctx")
    mine = lax.axis_index("ctx")
    heads_each = HEADS // parts
    totals = lax.dynamic_slice_in_dim(totals, mine * heads_each, heads_each, 1)
    factors = jnp.repeat(jnp.exp2(totals), HEAD_DIM, axis=1)[:, None, :]

    active = gather_project(rows, in_weight, filter_taps, filter_bias[None])
    states = device_states(active, gap_columns, ending_lanes, parts)
    owned = lax.all_to_all(states, "ctx", split_axis=0, concat_axis=0, tiled=True)
    running = jnp.zeros(owned.shape[1:], jnp.float32)
    entering = []
    for source in range(parts):
        entering.append(running.astype(jnp.bfloat16))
        running = running * factors[source] + owned[source].astype(jnp.float32)
    entering = lax.all_to_all(jnp.stack(entering), "ctx", split_axis=0, concat_axis=0, tiled=True)
    skip = jnp.repeat(skip_gain, HEAD_DIM)[None]
    return mix(
        active, decay_columns, gap_columns, gap_rows, ending_lanes, entering, skip, norm_gain[None]
    )[None]


def solution(mesh):
    in_specs = (P("dp", "ctx", None), P(None, "dp"), P(), P(), P(), P(), P(), P(), P())
    out_specs = P("dp", "ctx", None)
    return jax.shard_map(
        per_device, mesh=mesh, in_specs=in_specs, out_specs=out_specs, check_vma=False
    )
```

```python
import functools
import math

import jax
import jax.numpy as jnp
from jax import lax
from jax.experimental import pallas as pl
from jax.experimental.pallas import tpu as pltpu
from jax.sharding import PartitionSpec as P

HEADS = 64
HEAD_DIM = 64
STATE = 128
GROUPS = 4
BLOCK = 256
GROUP_HEADS = HEADS // GROUPS
GROUP_WIDTH = GROUP_HEADS * HEAD_DIM
INNER = HEADS * HEAD_DIM
RIM = 16
EXCHANGED = 16
LOG2E = math.log2(math.e)
VMEM_LIMIT = 60 * 2**20


CHUNKS = 4
SENT_ORDER = (2, 3, 0, 1)
TILE = 256


def flipped(index, bit):
    return index + bit - 2 * bit * ((index // bit) % 2)


def gather_project_kernel(
    rows_ref,
    weight_ref,
    taps_ref,
    bias_ref,
    active_ref,
    held,
    sums,
    local_sem,
    own_send,
    own_recv,
    x_send,
    x_recv,
    y_send,
    y_recv,
    z_send,
    z_recv,
    core_send,
    core_recv,
):
    me_dp, me_ctx = lax.axis_index("dp"), lax.axis_index("ctx")
    depth, width = weight_ref.shape
    length = active_ref.shape[0]
    quarter = depth // 4
    piece = quarter // CHUNKS
    partner, across, beyond = flipped(me_dp, 1), flipped(me_dp, 2), flipped(flipped(me_dp, 1), 2)
    core_peer, x_peer = (partner, me_ctx), (across, me_ctx)
    y_peer, z_peer = (me_dp, flipped(me_ctx, 1)), (me_dp, flipped(me_ctx, 2))
    mine = me_ctx % 4
    quarters = (mine, flipped(mine, 1), flipped(mine, 2), 3 - mine)

    barrier = pltpu.get_barrier_semaphore()
    for peer in (core_peer, x_peer, y_peer, z_peer):
        pl.semaphore_signal(
            barrier, inc=1, device_id=peer, device_id_type=pl.DeviceIdType.MESH
        )
    pl.semaphore_wait(barrier, 4)

    def span(kind, chunk):
        start = quarters[kind] * quarter + chunk * piece
        return pl.ds(pl.multiple_of(start, piece), piece)

    def remote(source, target, send, recv, peer):
        return pltpu.make_async_remote_copy(
            src_ref=source,
            dst_ref=target,
            send_sem=send,
            recv_sem=recv,
            device_id=peer,
            device_id_type=pl.DeviceIdType.MESH,
        )

    started = []

    def start(copy):
        copy.start()
        started.append(copy)

    local = pltpu.make_async_copy(weight_ref, held.at[me_dp], local_sem)
    local.start()
    start(remote(weight_ref, held.at[me_dp], own_send, own_recv, core_peer))
    x_slots = [(0, chunk) for chunk in SENT_ORDER] + [(3, 0), (3, 1)]
    for slot, (kind, chunk) in enumerate(x_slots):
        rows = span(kind, chunk)
        start(
            remote(
                weight_ref.at[rows, :],
                held.at[me_dp, rows, :],
                x_send.at[slot],
                x_recv.at[slot],
                x_peer,
            )
        )

    def landed(kind, chunk, recv, send, peer):
        part = held.at[across, span(kind, chunk), :]
        remote(part, part, send, recv, peer).wait_recv()

    def forward(kind, chunk, send, recv, peer):
        part = held.at[across, span(kind, chunk), :]
        start(remote(part, part, send, recv, peer))

    def to_core(kind, chunk):
        slot = kind * CHUNKS + chunk
        forward(kind, chunk, core_send.at[slot], core_recv.at[slot], core_peer)

    def from_x(slot):
        kind, chunk = x_slots[slot]
        landed(kind, chunk, x_recv.at[slot], x_send.at[slot], x_peer)
        if slot < CHUNKS:
            forward(kind, chunk, y_send.at[slot], y_recv.at[slot], y_peer)
            forward(kind, chunk, z_send.at[slot], z_recv.at[slot], z_peer)
        to_core(kind, chunk)

    def from_y(slot):
        kind, chunk = (1, SENT_ORDER[slot]) if slot < CHUNKS else (3, 3)
        landed(kind, chunk, y_recv.at[slot], y_send.at[slot], y_peer)
        if (kind, chunk) == (1, 2):
            forward(kind, chunk, z_send.at[CHUNKS], z_recv.at[CHUNKS], z_peer)
        to_core(kind, chunk)

    def from_z(slot):
        kind, chunk = (2, SENT_ORDER[slot]) if slot < CHUNKS else (3, 2)
        landed(kind, chunk, z_recv.at[slot], z_send.at[slot], z_peer)
        if (kind, chunk) == (2, 3):
            forward(kind, chunk, y_send.at[CHUNKS], y_recv.at[CHUNKS], y_peer)
        to_core(kind, chunk)

    def from_core(kind):
        for chunk in range(CHUNKS):
            part = held.at[beyond, span(kind, chunk), :]
            slot = kind * CHUNKS + chunk
            remote(part, part, core_send.at[slot], core_recv.at[slot], core_peer).wait_recv()

    def finish(total, shard, tile):
        lanes = pl.ds(pl.multiple_of(shard * width + tile * TILE, 128), TILE)
        projected = total.astype(jnp.bfloat16).astype(jnp.float32)
        taps = taps_ref[:, lanes]
        count = taps.shape[0]
        summed = bias_ref[:, lanes] + taps[count - 1 : count] * projected[RIM:]
        for k in range(count - 1):
            first = RIM - (count - 1) + k
            summed = summed + taps[k : k + 1] * projected[first : first + length]
        active_ref[:, lanes] = (summed / (1.0 + jnp.exp(-summed))).astype(jnp.bfloat16)

    def whole_shard(shard):
        @pl.loop(0, width // TILE)
        def _(tile):
            lanes = pl.ds(pl.multiple_of(tile * TILE, TILE), TILE)
            finish(
                jnp.dot(
                    rows_ref[...], held[shard, :, lanes], preferred_element_type=jnp.float32
                ),
                shard,
                tile,
            )

    def part_shard(shard, at, kinds, first, last):
        @pl.loop(0, width // TILE)
        def _(tile):
            lanes = pl.ds(pl.multiple_of(tile * TILE, TILE), TILE)
            total = None if first else sums[at, :, lanes]
            for kind in kinds:
                deep = pl.ds(pl.multiple_of(quarters[kind] * quarter, quarter), quarter)
                product = jnp.dot(
                    rows_ref[:, deep],
                    held[shard, deep, lanes],
                    preferred_element_type=jnp.float32,
                )
                total = product if total is None else total + product
            if last:
                finish(total, shard, tile)
            else:
                sums[at, :, lanes] = total

    local.wait()
    whole_shard(me_dp)
    from_x(0)
    remote(weight_ref, held.at[partner], own_send, own_recv, core_peer).wait_recv()
    whole_shard(partner)
    from_x(1)
    from_y(0)
    from_z(0)
    from_x(2)
    from_z(1)
    from_y(1)
    from_x(3)
    part_shard(across, 0, (0,), True, False)
    from_core(0)
    part_shard(beyond, 1, (0,), True, False)
    from_y(2)
    from_z(2)
    from_y(3)
    from_z(3)
    part_shard(across, 0, (1, 2), False, False)
    from_core(1)
    from_core(2)
    part_shard(beyond, 1, (1, 2), False, False)
    from_x(4)
    from_x(5)
    from_y(4)
    from_z(4)
    part_shard(across, 0, (3,), False, True)
    from_core(3)
    part_shard(beyond, 1, (3,), False, True)
    for copy in started:
        copy.wait_send()


def gather_project(rows, weight, taps, bias):
    length = rows.shape[0] - RIM
    depth, width = weight.shape
    shards = lax.axis_size("dp")
    dma = pltpu.SemaphoreType.DMA
    vmem = pl.BlockSpec(memory_space=pltpu.VMEM)
    return pl.pallas_call(
        gather_project_kernel,
        in_specs=[vmem, pl.BlockSpec(memory_space=pl.ANY), vmem, vmem],
        out_specs=vmem,
        out_shape=jax.ShapeDtypeStruct((length, shards * width), jnp.bfloat16),
        scratch_shapes=[
            pltpu.VMEM((shards, depth, width), jnp.bfloat16),
            pltpu.VMEM((2, length + RIM, width), jnp.float32),
            dma,
            dma,
            dma,
            dma((CHUNKS + 2,)),
            dma((CHUNKS + 2,)),
            dma((CHUNKS + 1,)),
            dma((CHUNKS + 1,)),
            dma((CHUNKS + 1,)),
            dma((CHUNKS + 1,)),
            dma((4 * CHUNKS,)),
            dma((4 * CHUNKS,)),
        ],
        compiler_params=pltpu.CompilerParams(
            vmem_limit_bytes=VMEM_LIMIT, collective_id=0, has_side_effects=True
        ),
        name="gather_project",
    )(rows, weight, taps, bias)


def pair_columns(columns, pair, low_half):
    first = 2 * pair
    return jnp.where(low_half, columns[:, first : first + 1], columns[:, first + 1 : first + 2])


def block_state(values, input_map, ending, gap_columns, low_half):
    pieces = []
    for pair in range(GROUP_HEADS // 2):
        lanes = slice(pair * 128, (pair + 1) * 128)
        weight = jnp.exp2(ending[:, lanes] - pair_columns(gap_columns, pair, low_half))
        pieces.append((weight * values[:, lanes].astype(jnp.float32)).astype(jnp.bfloat16))
    scaled = jnp.concatenate(pieces, axis=1)
    return lax.dot_general(
        input_map, scaled, (((0,), (0,)), ((), ())), preferred_element_type=jnp.float32
    )


def low_mask(rows):
    return lax.broadcasted_iota(jnp.int32, (rows, 128), 1) < HEAD_DIM


def states_kernel(values_ref, input_ref, gap_ref, ending_ref, state_ref):
    blocks = values_ref.shape[0] // BLOCK
    low_half = low_mask(BLOCK)
    total = None
    for k in range(blocks):
        rows = pl.ds(k * BLOCK, BLOCK)
        ending = ending_ref[k]
        state = block_state(values_ref[rows, :], input_ref[rows, :], ending, gap_ref[0, rows, :], low_half)
        total = state if total is None else total * jnp.exp2(ending) + state
    chunks, _, width = state_ref.shape
    for chunk in range(chunks):
        state_ref[chunk] = total[:, chunk * width : (chunk + 1) * width].astype(jnp.bfloat16)


def device_states(active, gap, ending, parts):
    length = active.shape[0]
    chunks = parts // GROUPS
    blocks = length // BLOCK
    width = INNER // parts
    return pl.pallas_call(
        states_kernel,
        grid=(GROUPS,),
        in_specs=[
            pl.BlockSpec((length, GROUP_WIDTH), lambda g: (0, g)),
            pl.BlockSpec((length, STATE), lambda g: (0, INNER // STATE + g)),
            pl.BlockSpec((1, length, GROUP_HEADS), lambda g: (g, 0, 0)),
            pl.BlockSpec((blocks, 1, GROUP_WIDTH), lambda g: (0, 0, g)),
        ],
        out_specs=pl.BlockSpec((chunks, STATE, width), lambda g: (g, 0, 0)),
        out_shape=jax.ShapeDtypeStruct((parts, STATE, width), jnp.bfloat16),
        compiler_params=pltpu.CompilerParams(vmem_limit_bytes=VMEM_LIMIT),
        name="states",
    )(active, active, gap, ending)


def mix_kernel(
    values_ref,
    input_ref,
    output_ref,
    decay_ref,
    gap_ref,
    gap_row_ref,
    ending_ref,
    entering_ref,
    skip_ref,
    gain_ref,
    normed_ref,
    entering_scratch,
    mixed_scratch,
):
    blocks = values_ref.shape[0] // BLOCK
    half = BLOCK // 2
    low_half = low_mask(BLOCK)
    causal = lax.broadcasted_iota(jnp.int32, (half, half), 0) >= lax.broadcasted_iota(
        jnp.int32, (half, half), 1
    )
    chunks, _, width = entering_ref.shape
    for chunk in range(chunks):
        entering_scratch[:, chunk * width : (chunk + 1) * width] = entering_ref[chunk].astype(jnp.float32)
    for k in range(blocks):
        rows = pl.ds(k * BLOCK, BLOCK)
        input_map = input_ref[rows, :]
        output_map = output_ref[rows, :]
        scores = lax.dot_general(
            output_map, input_map, (((1,), (1,)), ((), ())), preferred_element_type=jnp.float32
        )
        decay = decay_ref[0, rows, :]
        gap_rows = gap_row_ref[0, :, rows]
        carried = jnp.dot(
            output_map, entering_scratch[...].astype(jnp.bfloat16), preferred_element_type=jnp.float32
        )
        squares = jnp.zeros((BLOCK, 128), jnp.float32)
        for pair in range(GROUP_HEADS // 2):
            lanes = slice(pair * 128, (pair + 1) * 128)
            values = values_ref[rows, lanes]
            within = []
            for head in (2 * pair, 2 * pair + 1):
                column = decay[:, head : head + 1]
                row = gap_rows[head : head + 1, :]
                top = jnp.where(causal, column[:half] - row[:, :half], -jnp.inf)
                top = (jnp.exp2(top) * scores[:half, :half]).astype(jnp.bfloat16)
                left = jnp.exp2(column[half:] - row[:, :half]) * scores[half:, :half]
                right = jnp.where(causal, column[half:] - row[:, half:], -jnp.inf)
                right = jnp.exp2(right) * scores[half:, half:]
                bottom = jnp.concatenate([left, right], axis=1).astype(jnp.bfloat16)
                within.append(
                    jnp.concatenate(
                        [
                            jnp.dot(top, values[:half], preferred_element_type=jnp.float32),
                            jnp.dot(bottom, values, preferred_element_type=jnp.float32),
                        ],
                        axis=0,
                    )
                )
            inside = jnp.where(low_half, within[0], within[1])
            growth = jnp.exp2(pair_columns(decay, pair, low_half))
            mixed = (
                inside
                + growth * carried[:, lanes]
                + skip_ref[:, lanes] * values.astype(jnp.float32)
            ).astype(jnp.bfloat16)
            mixed_scratch[:, lanes] = mixed
            wide = mixed.astype(jnp.float32)
            squares = squares + wide * wide
        mean = jnp.sum(squares, axis=1, keepdims=True) * (1.0 / GROUP_WIDTH)
        scale = lax.rsqrt(mean + 1e-05)
        normed_ref[rows, :] = (
            mixed_scratch[...].astype(jnp.float32) * scale * gain_ref[...]
        ).astype(jnp.bfloat16)
        if k < blocks - 1:
            ending = ending_ref[k]
            state = block_state(values_ref[rows, :], input_map, ending, gap_ref[0, rows, :], low_half)
            entering_scratch[...] = entering_scratch[...] * jnp.exp2(ending) + state


def mix(active, decay, gap, gap_rows, ending, entering, skip, gain):
    length = active.shape[0]
    blocks = length // BLOCK
    parts, _, width = entering.shape
    chunks = parts // GROUPS
    group_column = lambda g: (0, g)
    return pl.pallas_call(
        mix_kernel,
        grid=(GROUPS,),
        in_specs=[
            pl.BlockSpec((length, GROUP_WIDTH), group_column),
            pl.BlockSpec((length, STATE), lambda g: (0, INNER // STATE + g)),
            pl.BlockSpec((length, STATE), lambda g: (0, INNER // STATE + GROUPS + g)),
            pl.BlockSpec((1, length, GROUP_HEADS), lambda g: (g, 0, 0)),
            pl.BlockSpec((1, length, GROUP_HEADS), lambda g: (g, 0, 0)),
            pl.BlockSpec((1, GROUP_HEADS, length), lambda g: (g, 0, 0)),
            pl.BlockSpec((blocks, 1, GROUP_WIDTH), lambda g: (0, 0, g)),
            pl.BlockSpec((chunks, STATE, width), lambda g: (g, 0, 0)),
            pl.BlockSpec((1, GROUP_WIDTH), group_column),
            pl.BlockSpec((1, GROUP_WIDTH), group_column),
        ],
        out_specs=pl.BlockSpec((length, GROUP_WIDTH), group_column),
        out_shape=jax.ShapeDtypeStruct((length, INNER), jnp.bfloat16),
        scratch_shapes=[
            pltpu.VMEM((STATE, GROUP_WIDTH), jnp.float32),
            pltpu.VMEM((BLOCK, GROUP_WIDTH), jnp.bfloat16),
        ],
        compiler_params=pltpu.CompilerParams(vmem_limit_bytes=VMEM_LIMIT),
        name="mix",
    )(active, active, active, decay, gap, gap_rows, ending, entering, skip, gain)


def exchange_kernel(
    state_ref,
    factor_ref,
    entering_ref,
    other_state,
    other_factor,
    arriving,
    leaving,
    answer,
    factor_send,
    factor_recv,
    state_send,
    state_recv,
    chain_send,
    chain_recv,
    answer_send,
    answer_recv,
):
    me_dp, me = lax.axis_index("dp"), lax.axis_index("ctx")
    count = lax.axis_size("ctx")
    half = other_state.shape[0]
    parity = me % 2
    first, other_first = parity * half, (1 - parity) * half
    partner = (me_dp, flipped(me, 1))
    after, before = (me_dp, (me + 2) % count), (me_dp, (me + count - 2) % count)

    barrier = pltpu.get_barrier_semaphore()
    for peer in (partner, after, before):
        pl.semaphore_signal(
            barrier, inc=1, device_id=peer, device_id_type=pl.DeviceIdType.MESH
        )
    pl.semaphore_wait(barrier, 3)

    def remote(source, target, send, recv, peer):
        return pltpu.make_async_remote_copy(
            src_ref=source,
            dst_ref=target,
            send_sem=send,
            recv_sem=recv,
            device_id=peer,
            device_id_type=pl.DeviceIdType.MESH,
        )

    factors = remote(
        factor_ref.at[pl.ds(other_first, half)], other_factor, factor_send, factor_recv, partner
    )
    factors.start()
    shared, chained, answers = [], [], []
    for i in range(half):
        shared.append(
            remote(
                state_ref.at[other_first + i],
                other_state.at[i],
                state_send.at[i],
                state_recv.at[i],
                partner,
            )
        )
        shared[i].start()
        chained.append(
            remote(leaving.at[i], arriving.at[i], chain_send.at[i], chain_recv.at[i], after)
        )
        answers.append(
            remote(
                answer.at[i],
                entering_ref.at[first + i],
                answer_send.at[i],
                answer_recv.at[i],
                partner,
            )
        )

    @pl.when(me < 2)
    def _():
        arriving[...] = jnp.zeros_like(arriving)

    factors.wait_recv()
    even = parity == 0
    for i in range(half):
        shared[i].wait_recv()

        @pl.when(me >= 2)
        def _():
            chained[i].wait_recv()

        own, theirs = state_ref[first + i].astype(jnp.float32), other_state[i].astype(jnp.float32)
        own_factor, their_factor = factor_ref[first + i], other_factor[i]
        early, late = jnp.where(even, own, theirs), jnp.where(even, theirs, own)
        early_factor = jnp.where(even, own_factor, their_factor)
        late_factor = jnp.where(even, their_factor, own_factor)
        start = arriving[i].astype(jnp.float32)
        middle = start * early_factor + early
        leaving[i] = (middle * late_factor + late).astype(jnp.bfloat16)

        @pl.when(me < count - 2)
        def _():
            chained[i].start()

        answer[i] = jnp.where(even, middle, start).astype(jnp.bfloat16)
        answers[i].start()
        entering_ref[first + i] = jnp.where(even, start, middle).astype(jnp.bfloat16)

    for i in range(half):
        remote(
            answer.at[i],
            entering_ref.at[other_first + i],
            answer_send.at[i],
            answer_recv.at[i],
            partner,
        ).wait_recv()
        shared[i].wait_send()
        answers[i].wait_send()

        @pl.when(me < count - 2)
        def _():
            chained[i].wait_send()

    factors.wait_send()


def exchange(states, factors):
    parts = states.shape[0]
    half = parts // 2
    dma = pltpu.SemaphoreType.DMA
    vmem = pl.BlockSpec(memory_space=pltpu.VMEM)
    piece = (half,) + states.shape[1:]
    return pl.pallas_call(
        exchange_kernel,
        in_specs=[vmem, vmem],
        out_specs=vmem,
        out_shape=jax.ShapeDtypeStruct(states.shape, jnp.bfloat16),
        scratch_shapes=[
            pltpu.VMEM(piece, jnp.bfloat16),
            pltpu.VMEM((half,) + factors.shape[1:], jnp.float32),
            pltpu.VMEM(piece, jnp.bfloat16),
            pltpu.VMEM(piece, jnp.bfloat16),
            pltpu.VMEM(piece, jnp.bfloat16),
            dma,
            dma,
        ]
        + [dma((half,))] * 6,
        compiler_params=pltpu.CompilerParams(
            vmem_limit_bytes=VMEM_LIMIT, collective_id=1, has_side_effects=True
        ),
        name="exchange",
    )(states, factors)


def per_device(
    tokens,
    in_weight,
    step_weight,
    step_bias,
    decay_rate,
    skip_gain,
    filter_taps,
    filter_bias,
    norm_gain,
):
    token_rows = tokens[0]
    length = token_rows.shape[0]
    blocks = length // BLOCK
    parts = lax.axis_size("ctx")
    rim = lax.ppermute(token_rows[length - RIM :], "ctx", [(s, s + 1) for s in range(parts - 1)])
    rows = jnp.concatenate([rim, token_rows], axis=0)

    step_raw = jnp.dot(token_rows, step_weight, preferred_element_type=jnp.float32).astype(
        jnp.bfloat16
    )
    step_size = jax.nn.softplus(step_raw.astype(jnp.float32) + step_bias)
    decay = jnp.cumsum((-step_size * decay_rate).reshape(blocks, BLOCK, HEADS), axis=1) * LOG2E
    ending = decay[:, -1, :]
    decay = decay.reshape(length, HEADS)
    gap = decay - jnp.log2(step_size)
    grouped = lambda array: array.reshape(length, GROUPS, GROUP_HEADS).transpose(1, 0, 2)
    decay_columns, gap_columns = grouped(decay), grouped(gap)
    gap_rows = gap.T.reshape(GROUPS, GROUP_HEADS, length)
    ending_lanes = jnp.repeat(ending, HEAD_DIM, axis=1)[:, None, :]
    parts_width = INNER // EXCHANGED
    factors = jnp.repeat(jnp.exp2(jnp.sum(ending, axis=0)), HEAD_DIM)
    factors = factors.reshape(EXCHANGED, 1, parts_width)

    active = gather_project(rows, in_weight, filter_taps, filter_bias[None])
    states = device_states(active, gap_columns, ending_lanes, EXCHANGED)
    entering = exchange(states, factors)
    skip = jnp.repeat(skip_gain, HEAD_DIM)[None]
    return mix(
        active, decay_columns, gap_columns, gap_rows, ending_lanes, entering, skip, norm_gain[None]
    )[None]


def solution(mesh):
    in_specs = (P("dp", "ctx", None), P(None, "dp"), P(), P(), P(), P(), P(), P(), P())
    out_specs = P("dp", "ctx", None)
    return jax.shard_map(
        per_device, mesh=mesh, in_specs=in_specs, out_specs=out_specs, check_vma=False
    )
```
